32 devices in a mesh: grp: 4 (over z), row: 8 (over y, x, core).
Axes of the slice: x: 2, y: 2, z: 4, core: 2. Of those that a mesh axis runs over, the one named last changes fastest.
Arguments:
- a_pieces: bfloat16 [4, 512, 4096], P('grp', 'row'), as said below
- touched: int32 [4, 512], P('grp', 'row'), may hold values from 0 to 7
- slot_row: int32 [512], P('row'), may hold values from 0 to 511, as said below
- x_blocks: bfloat16 [32, 64, 64], P('grp'), as said below
- z_inverse: bfloat16 [32, 64, 64], P('grp'), as said below
- block_class: int32 [32], P('grp'), may hold values from 0 to 1
Outputs:
- schur: float32 [512, 512], P('row', 'grp')
The draws below stay inside these ranges and needn't reach their ends.
Inputs may be any that keep to these rules, and one draw needn't show every extreme that they name: `slot_row`: A permutation of the constraints. The 64 slots of one index r of row (slots r * 64 onward) hold, of the constraints o * 64 to (o + 1) * 64 - 1 of each index o, either none or exactly 16. `a_pieces`: each piece read as a 64 x 64 matrix is symmetric. `x_blocks`: each block is symmetric positive definite. `z_inverse`: each block is symmetric positive definite.
All inputs are finite; a program needn't handle non-finite values.
Results may differ from the reference program's by a relative error of at most 0.0008.
Values may be sent and summed in bfloat16 or wider, within the bound.
A program may use at most 64 MiB of HBM per device.

```python
import math
import jax
import jax.numpy as jnp
import numpy as np
from jax import lax

NB = 64
BLK_DEV = 8
ROWS_DEV = 64
CAP = 16
M = 512
BLOCKS = 32
N_GRP = 4


def definite_blocks(key):
    raw = jax.random.normal(key, (BLOCKS, NB, NB), jnp.float32) / math.sqrt(NB)
    gram = jnp.einsum('kab,kcb->kac', raw, raw, precision=lax.Precision.HIGHEST)
    gram = 0.5 * (gram + jnp.swapaxes(gram, 1, 2)) + 0.5 * jnp.eye(NB, dtype=jnp.float32)[None]
    return gram.astype(jnp.bfloat16)


def draw_x_blocks(key, part):
    return definite_blocks(jax.random.fold_in(key, 11))


def draw_z_inverse(key, part):
    return definite_blocks(jax.random.fold_in(key, 23))


def draw_a_pieces(key, part):
    groups = BLOCKS // BLK_DEV
    raw = jax.random.normal(jax.random.fold_in(key, 31), (groups, M, NB, NB), jnp.float32)
    symmetric = (raw + jnp.swapaxes(raw, 2, 3)) / math.sqrt(2.0) / math.sqrt(8.0 * NB)
    return symmetric.reshape(groups, M, NB * NB).astype(jnp.bfloat16)


def shuffled(subkey):
    return jax.random.permutation(subkey, ROWS_DEV)


def place_value(order, value, position):
    where_now = jnp.argmax((order == value).astype(jnp.int32)).astype(jnp.int32)
    displaced = order[position]
    order = order.at[where_now].set(displaced)
    return order.at[position].set(value)


def draw_slot_row(key, part):
    devices = M // ROWS_DEV
    key_one, key_two = jax.random.split(jax.random.fold_in(key, 41))
    mixed = jax.random.permutation(key_one, devices)
    rotated = (mixed - mixed[0] + devices // 2) % devices
    rotated = place_value(rotated, 1, 1)
    rotated = place_value(rotated, devices - 1, 2)
    shifts = rotated[:ROWS_DEV // CAP]
    offsets = jnp.repeat(shifts, CAP)
    orders = jax.vmap(shuffled)(jax.random.split(key_two, devices))
    sources = jnp.arange(devices, dtype=jnp.int32)[:, None]
    owners = (sources - offsets[orders]) % devices
    return (owners * ROWS_DEV + orders).reshape(-1).astype(jnp.int32)


def with_ends(drawn, rng, smallest, high):
    longest = drawn.shape.index(max(drawn.shape))
    spots = []
    for shift in (0, 1):
        where = [jax.random.randint(jax.random.fold_in(rng, axis), (), 0, length) for axis, length in enumerate(drawn.shape)]
        where[longest] = (where[longest] + shift) % drawn.shape[longest]
        spots.append(tuple(where))
    return drawn.at[spots[0]].set(smallest).at[spots[1]].set(high)


def cumulative_ranks(amount, skew):
    weights = [(1 << 20) // math.isqrt(standing ** skew) + 1 for standing in range(1, amount + 1)]
    scale = 1 + sum(weights) // (1 << 30)
    return np.cumsum(np.array([max(1, weight // scale) for weight in weights]))


def ranked_ids(key, dims, count, slope):
    grid = cumulative_ranks(count, slope)
    lot = jax.random.randint(jax.random.fold_in(key, 1), dims, 0, int(grid[count - 1]))
    rank = jnp.searchsorted(jnp.asarray(grid, jnp.int32), lot, side="right")
    return jax.random.permutation(jax.random.fold_in(key, 2), count)[rank].astype(jnp.int32)


def setup_inputs(seed: int = 0) -> dict:
    splits = jax.random.split(jax.random.key(seed), 7)
    a_pieces = draw_a_pieces(jax.random.fold_in(splits[6], 71), 0)
    touched = with_ends(ranked_ids(splits[1], (N_GRP, M), BLK_DEV, 2), jax.random.fold_in(splits[1], 3), 0, BLK_DEV - 1).astype(jnp.int32)
    slot_row = draw_slot_row(jax.random.fold_in(splits[6], 71), 0)
    x_blocks = draw_x_blocks(jax.random.fold_in(splits[6], 71), 0)
    z_inverse = draw_z_inverse(jax.random.fold_in(splits[6], 71), 0)
    block_class = with_ends(jax.random.randint(splits[5], (BLOCKS,), 0, 2), jax.random.fold_in(splits[5], 1), 0, 1).astype(jnp.int32)
    return {"a_pieces": a_pieces, "touched": touched, "slot_row": slot_row, "x_blocks": x_blocks, "z_inverse": z_inverse, "block_class": block_class}


def masked_blocks(blocks, block_class):
    positions = jnp.arange(NB)
    active = (NB // 2) * (1 + block_class)
    inside = (positions[None, :, None] < active[:, None, None]) & (positions[None, None, :] < active[:, None, None])
    return jnp.where(inside, blocks, jnp.zeros_like(blocks))


def reference(a_pieces, touched, slot_row, x_blocks, z_inverse, block_class):
    x_masked = masked_blocks(x_blocks, block_class).reshape(N_GRP, BLK_DEV, NB, NB)
    z_masked = masked_blocks(z_inverse, block_class).reshape(N_GRP, BLK_DEV, NB, NB)

    def group_step(running, group_args):
        a_group, group_kinds, x_group, z_group = group_args
        pieces = a_group.reshape(M, NB, NB).astype(jnp.float32)
        left_part = jnp.einsum("rab,rbc->rac", x_group[group_kinds].astype(jnp.float32), pieces,
                               precision=lax.Precision.HIGHEST).astype(jnp.bfloat16)
        product = jnp.einsum("rab,rbc->rac", left_part.astype(jnp.float32), z_group[group_kinds].astype(jnp.float32),
                             precision=lax.Precision.HIGHEST).astype(jnp.bfloat16)
        scores = jnp.dot(product.reshape(M, NB * NB).astype(jnp.float32), a_group.astype(jnp.float32).T,
                         precision=lax.Precision.HIGHEST)
        scores = jnp.where(group_kinds[:, None] == group_kinds[None, :], scores, jnp.zeros_like(scores))
        return running + scores, None

    start_sum = jnp.zeros((M, M), jnp.float32)
    schur_slots, unused = lax.scan(group_step, start_sum, (a_pieces, touched, x_masked, z_masked))
    inverse = jnp.zeros((M,), jnp.int32).at[slot_row].set(jnp.arange(M, dtype=jnp.int32))
    return schur_slots[inverse][:, inverse]
```

```python
import functools
import jax
import jax.numpy as jnp
from jax import lax
from jax.experimental import pallas as pl
from jax.experimental.pallas import tpu as pltpu
from jax.sharding import PartitionSpec as P

F32, BF16, I32 = jnp.float32, jnp.bfloat16, jnp.int32
LANES = 128


def iota(shape, dim):
    return lax.broadcasted_iota(I32, shape, dim)


def mm(a, b):
    return lax.dot_general(a, b, (((1,), (0,)), ((), ())), preferred_element_type=F32)


def mm_nt(a, b):
    return lax.dot_general(a, b, (((1,), (1,)), ((), ())), preferred_element_type=F32)


def split(v):
    hi = v.astype(BF16)
    return hi, (v - hi.astype(F32)).astype(BF16)


def onehot(mask):
    return jnp.where(mask, 1.0, 0.0).astype(BF16)


def kernel(
    n, ng, cap,
    a_ref, touched_s, class_s, touched_v, slot_v, x_ref, z_ref,
    out_ref,
    gath, meta, w_ref, zm_ref, l3, p3, q_ref, score, zsend, zrecv, osend, orecv,
    g_send, g_recv, m_send, m_recv, z_ssem, z_rsem, o_send, o_recv,
):
    rows, flat = a_ref.shape[1], a_ref.shape[2]
    kinds, nb = x_ref.shape[0], x_ref.shape[1]
    half = nb // 2
    tiles = flat // LANES
    fold = tiles // 2
    hrows = rows // 2
    pairs = n // 2
    cols = out_ref.shape[1]
    g, me = lax.axis_index("grp"), lax.axis_index("row")

    def rdma(src, dst, ssem, rsem, dev):
        return pltpu.make_async_remote_copy(
            src_ref=src, dst_ref=dst, send_sem=ssem, recv_sem=rsem,
            device_id=dev, device_id_type=pl.DeviceIdType.MESH,
        )

    def row_peer(d):
        return lax.rem(me + d, n)

    def grp_peer(d):
        return lax.rem(g + d, ng)

    barrier = pltpu.get_barrier_semaphore()
    for d in range(1, n):
        pl.semaphore_signal(
            barrier, inc=1, device_id=(g, row_peer(d)), device_id_type=pl.DeviceIdType.MESH
        )
    for d in range(1, ng):
        pl.semaphore_signal(
            barrier, inc=1, device_id=(grp_peer(d), me), device_id_type=pl.DeviceIdType.MESH
        )

    lane = iota((rows, LANES), 1)
    in_row = lax.rem(lane, nb)
    second = (lane >= nb).astype(I32)

    def pack(top, bottom, t):
        turned = pltpu.roll(bottom, LANES - half, 1)
        return jnp.where(in_row < 2 * t + second, turned, top)

    def diagonal(bottom, t):
        hit = in_row == half + 2 * t + second
        return jnp.where(hit, bottom, 0.0)

    extra = jnp.zeros((rows, LANES), F32)
    for t in range(fold):
        top = a_ref[0, :, t * LANES:(t + 1) * LANES].astype(F32)
        bottom = a_ref[0, :, (t + fold) * LANES:(t + fold + 1) * LANES].astype(F32)
        gath[me, :, t * LANES:(t + 1) * LANES] = pack(top, bottom, t).astype(BF16)
        extra = extra + diagonal(bottom, t)
    gath[me, :, fold * LANES:(fold + 1) * LANES] = extra.astype(BF16)

    core = lax.rem(me, 2)
    meta[me] = jnp.full((8, LANES), -1, I32)
    meta[me, 0:1, 0:rows] = touched_v[...]
    meta[me, 1:2, 0:rows] = slot_v[...]
    own_meta = meta[me]
    own_touched = own_meta[0:1, :]
    own_slot = own_meta[1:2, :]
    meta[me] = jnp.where(core == 1, pltpu.roll(own_meta, rows, 1), own_meta)

    pl.semaphore_wait(barrier, n - 1 + ng - 1)

    started = []

    def go(src, dst, ssem, rsem, dev):
        c = rdma(src, dst, ssem, rsem, dev)
        c.start()
        started.append(c)

    counter = [0]

    def send_half(s, h, dst_row):
        k = counter[0]
        counter[0] += 1
        view = gath.at[s, pl.ds(h * hrows, hrows)]
        go(view, view, g_send.at[k], g_recv.at[s, h], (g, dst_row))

    def wait_half(s, h):
        view = gath.at[s, pl.ds(h * hrows, hrows)]
        rdma(view, view, g_send.at[0], g_recv.at[s, h], (g, row_peer(1))).wait_recv()

    relay = n == 8
    if relay:
        def flip(v, bit):
            return v + bit - 2 * bit * lax.rem(lax.div(v, bit), 2)
        sib, xn, yn = flip(me, 1), flip(me, 2), flip(me, 4)
        dn = flip(xn, 4)
        send_half(me, 0, xn)
        send_half(me, 1, yn)
        send_half(me, 1, xn)
        send_half(me, 0, yn)
        send_half(me, 0, sib)
        send_half(me, 1, sib)
    else:
        for d in range(1, n):
            for h in range(2):
                send_half(me, h, row_peer(d))
    for d in range(1, n):
        go(meta.at[me], meta.at[me], m_send.at[d], m_recv.at[me], (g, row_peer(d)))

    r64, c64 = iota((nb, nb), 0), iota((nb, nb), 1)
    dup = onehot(lax.rem(iota((nb, LANES), 1), nb) == iota((nb, LANES), 0))
    lane_b = iota((nb, LANES), 1)
    for k in range(kinds):
        active = half * (1 + class_s[k])
        inside = (r64 < active) & (c64 < active)
        xm = jnp.where(inside, x_ref[k].astype(F32), 0.0).astype(BF16)
        zm_ref[k] = jnp.where(inside, z_ref[k].astype(F32), 0.0).astype(BF16)
        wide = mm(xm, dup)
        w_ref[0:nb, k * LANES:(k + 1) * LANES] = jnp.where(lane_b < nb, wide, 0.0).astype(BF16)
        w_ref[nb:2 * nb, k * LANES:(k + 1) * LANES] = jnp.where(lane_b >= nb, wide, 0.0).astype(BF16)

    spread = jnp.broadcast_to(own_touched, (LANES, LANES)).astype(F32)
    own_kind = jnp.transpose(spread)[0:rows, :]

    def left_tile(t, carry):
        off = pl.multiple_of(t * LANES, LANES)
        at = a_ref[0, :, pl.ds(off, LANES)]
        full = mm(at, w_ref[...])
        acc = jnp.zeros((rows, LANES), F32)
        for k in range(kinds):
            acc = acc + jnp.where(own_kind == k, full[:, k * LANES:(k + 1) * LANES], 0.0)
        acc = acc.astype(BF16).astype(F32)
        l3[pl.ds(2 * t, rows, stride=nb), :] = acc
        l3[pl.ds(2 * t + 1, rows, stride=nb), :] = pltpu.roll(acc, nb, 1)
        return carry

    def left_tiles(u, carry):
        for v in range(4):
            left_tile(u * 4 + v, carry)
        return carry

    lax.fori_loop(0, tiles // 4, left_tiles, 0)

    eye = onehot(r64 == c64)

    def product_step(u, carry):
        for v in range(8):
            i = u * 8 + v
            off = pl.multiple_of(i * nb, nb)
            lt = l3[pl.ds(off, nb), 0:nb].astype(BF16)
            zk = zm_ref[touched_s[0, i]]
            pt = mm(zk, lt).astype(BF16)
            ptf = pt.astype(F32)
            p3[pl.ds(off, nb), 0:nb] = jnp.where(r64 == c64, ptf, ptf + mm_nt(eye, pt))
        return carry

    steps = rows // 8
    if relay:
        lax.fori_loop(0, steps // 2, product_step, 0)
        wait_half(xn, 0)
        send_half(xn, 0, yn)
        send_half(xn, 0, sib)
        wait_half(yn, 1)
        send_half(yn, 1, xn)
        send_half(yn, 1, sib)
        lax.fori_loop(steps // 2, steps, product_step, 0)
        wait_half(xn, 1)
        send_half(xn, 1, sib)
        wait_half(yn, 0)
        send_half(yn, 0, sib)
    else:
        lax.fori_loop(0, steps, product_step, 0)

    low_lane = lane < nb
    qextra = jnp.zeros((rows, LANES), F32)

    def put(t, v):
        hi, lo = split(v)
        q_ref[0:rows, t * LANES:(t + 1) * LANES] = hi
        q_ref[rows:2 * rows, t * LANES:(t + 1) * LANES] = lo

    def flat_tile(t):
        even = p3[pl.ds(2 * t, rows, stride=nb), :]
        odd = p3[pl.ds(2 * t + 1, rows, stride=nb), :]
        return jnp.where(low_lane, even, pltpu.roll(odd, nb, 1))

    for t in range(fold):
        top, bottom = flat_tile(t), flat_tile(t + fold)
        put(t, pack(top, bottom, t))
        qextra = qextra + diagonal(bottom, t)
    put(fold, qextra)

    for d in range(1, n):
        s = row_peer(d)
        rdma(meta.at[s], meta.at[s], m_send.at[d], m_recv.at[s], (g, s)).wait_recv()

    def pair_meta(p):
        return jnp.maximum(meta[2 * p], meta[2 * p + 1])

    def score_pair(p):
        block = gath[pl.ds(2 * p, 2)].reshape(2 * rows, gath.shape[2])
        s = mm_nt(q_ref[...], block)
        s = s[0:rows] + s[rows:2 * rows]
        kind = pair_meta(p)[0:1, :].astype(F32)
        score[p] = jnp.where(own_kind == kind, s, 0.0)

    mine = lax.div(me, 2)
    if relay:
        wait_half(sib, 0)
        wait_half(sib, 1)
        score_pair(mine)
        sx, sy, sd = flip(sib, 2), flip(sib, 4), flip(flip(sib, 2), 4)
        wait_half(sx, 0)
        wait_half(sx, 1)
        score_pair(lax.div(xn, 2))
        wait_half(dn, 0)
        send_half(dn, 0, sib)
        wait_half(dn, 1)
        send_half(dn, 1, sib)
        wait_half(sy, 0)
        wait_half(sy, 1)
        score_pair(lax.div(yn, 2))
        wait_half(sd, 0)
        wait_half(sd, 1)
        score_pair(lax.div(dn, 2))
    else:
        for d in range(1, n):
            for h in range(2):
                wait_half(row_peer(d), h)

        def each(p, carry):
            score_pair(p)
            return carry

        lax.fori_loop(0, pairs, each, 0)

    def column_slice(q):
        def body(p, acc):
            want = q * cols + iota((cols, LANES), 0)
            table = onehot(pair_meta(p)[1:2, :] == want)
            hi, lo = split(score[p])
            both = mm_nt(jnp.concatenate([hi, lo], axis=0), table)
            return acc + both[0:rows] + both[rows:2 * rows]
        acc = jnp.zeros((rows, cols), F32)
        if pairs <= 4:
            for p in range(pairs):
                acc = body(p, acc)
            return acc
        return lax.fori_loop(0, pairs, body, acc)

    for d in range(1, ng):
        q = grp_peer(d)
        zsend[d] = column_slice(q)
        go(zsend.at[d], zrecv.at[g], z_ssem.at[d], z_rsem.at[g], (q, me))
    total = column_slice(g)

    i0, i1 = iota((LANES, LANES), 0), iota((LANES, LANES), 1)
    before = onehot((i0 < i1) & ((i0 < rows) == (i1 < rows)))
    o_id = iota((n, LANES), 0)
    owner = (own_slot >= o_id * rows) & (own_slot < (o_id + 1) * rows)
    owner_f = jnp.where(owner, 1.0, 0.0)
    rank = mm(onehot(owner), before)
    place = jnp.where(owner, rank + (o_id * cap).astype(F32) + 1.0, 0.0)
    place = jnp.sum(place, axis=0, keepdims=True).astype(I32) - 1
    route = onehot(iota((n * cap, LANES), 0) == place)[:, 0:rows]

    def landing(p):
        slots = pair_meta(p)[1:2, :]
        arrives = (slots >= me * rows) & (slots < (me + 1) * rows)
        arr = jnp.broadcast_to(jnp.where(arrives, 1.0, 0.0), (8, LANES)).astype(BF16)
        rank_in = mm(arr, before)[0:1, :].astype(I32)
        upper = (iota((1, LANES), 1) >= rows).astype(I32)
        at = jnp.where(arrives, rank_in + upper * cap, -1)
        pick = onehot(iota((2 * cap, LANES), 0) == at)
        where_to = onehot(slots == me * rows + iota((rows, LANES), 0))
        return mm_nt(where_to, pick).astype(BF16)

    lands = [landing(p) for p in range(pairs)]

    for d in range(1, ng):
        s = grp_peer(d)
        rdma(zsend.at[d], zrecv.at[s], z_ssem.at[d], z_rsem.at[s], (s, me)).wait_recv()
        total = total + zrecv[s]

    hi, lo = split(total)
    osend[...] = (mm(route, hi) + mm(route, lo)).reshape(osend.shape)
    for d in range(1, n):
        o = row_peer(d)
        go(osend.at[o], orecv.at[me], o_send.at[d], o_recv.at[me], (g, o))
    orecv[me] = osend[me]
    for d in range(1, n):
        s = row_peer(d)
        rdma(osend.at[s], orecv.at[s], o_send.at[d], o_recv.at[s], (g, s)).wait_recv()
    result = jnp.zeros((rows, cols), F32)
    for p in range(pairs):
        hi, lo = split(orecv[2 * p:2 * p + 2].reshape(2 * cap, cols))
        result = result + mm(lands[p], hi) + mm(lands[p], lo)
    out_ref[...] = result
    for c in started:
        c.wait_send()


def shards(n, ng, a_pieces, touched, slot_row, x_blocks, z_inverse, block_class):
    rows, flat = a_pieces.shape[1], a_pieces.shape[2]
    kinds, nb = x_blocks.shape[0], x_blocks.shape[1]
    packed = (flat // LANES // 2 + 1) * LANES
    cols = rows * n // ng
    cap = -(-max(2, rows // n * 2) // 8) * 8
    sends = 14 if n == 8 else 2 * n
    vmem = pl.BlockSpec(memory_space=pltpu.VMEM)
    smem = pl.BlockSpec(memory_space=pltpu.SMEM)
    dma = pltpu.SemaphoreType.DMA
    return pl.pallas_call(
        functools.partial(kernel, n, ng, cap),
        out_shape=jax.ShapeDtypeStruct((rows, cols), F32),
        in_specs=[vmem, smem, smem, vmem, vmem, vmem, vmem],
        out_specs=vmem,
        scratch_shapes=[
            pltpu.VMEM((n, rows, packed), BF16),
            pltpu.VMEM((n, 8, LANES), I32),
            pltpu.VMEM((2 * nb, kinds * LANES), BF16),
            pltpu.VMEM((kinds, nb, nb), BF16),
            pltpu.VMEM((rows * nb, LANES), F32),
            pltpu.VMEM((rows * nb, LANES), F32),
            pltpu.VMEM((2 * rows, packed), BF16),
            pltpu.VMEM((n // 2, rows, LANES), F32),
            pltpu.VMEM((ng, rows, cols), F32),
            pltpu.VMEM((ng, rows, cols), F32),
            pltpu.VMEM((n, cap, cols), F32),
            pltpu.VMEM((n, cap, cols), F32),
            dma((sends,)), dma((n, 2)), dma((n,)), dma((n,)),
            dma((ng,)), dma((ng,)), dma((n,)), dma((n,)),
        ],
        compiler_params=pltpu.CompilerParams(
            collective_id=0, has_side_effects=True, vmem_limit_bytes=56 * 1024 * 1024
        ),
    )(a_pieces, touched, block_class, touched, slot_row.reshape(1, rows), x_blocks, z_inverse)


def solution(mesh):
    n, ng = mesh.shape["row"], mesh.shape["grp"]
    return jax.shard_map(
        functools.partial(shards, n, ng),
        mesh=mesh,
        in_specs=(
            P("grp", "row", None),
            P("grp", "row"),
            P("row"),
            P("grp", None, None),
            P("grp", None, None),
            P("grp"),
        ),
        out_specs=P("row", "grp"),
        check_vma=False,
    )
```

```python
import functools
import jax
import jax.numpy as jnp
from jax import lax
from jax.experimental import pallas as pl
from jax.experimental.pallas import tpu as pltpu
from jax.sharding import PartitionSpec as P

F32, BF16, I32 = jnp.float32, jnp.bfloat16, jnp.int32
LANES = 128


def iota(shape, dim):
    return lax.broadcasted_iota(I32, shape, dim)


def mm(a, b):
    return lax.dot_general(a, b, (((1,), (0,)), ((), ())), preferred_element_type=F32)


def mm_nt(a, b):
    return lax.dot_general(a, b, (((1,), (1,)), ((), ())), preferred_element_type=F32)


def split(v):
    hi = v.astype(BF16)
    return hi, (v - hi.astype(F32)).astype(BF16)


def onehot(mask):
    return jnp.where(mask, 1.0, 0.0).astype(BF16)


def kernel(
    n, ng, cap,
    a_hbm, touched_hbm, class_s, slot_hbm, x_hbm, z_hbm,
    out_ref,
    a_ref, touched_s, touched_v, slot_v, x_ref, z_ref, in_sem,
    gath, meta, w_ref, zm_ref, l3, p3, q_ref, score, zsend, zrecv, osend, orecv,
    g_send, g_recv, m_send, m_recv, z_ssem, z_rsem, o_send, o_recv,
):
    rows, flat = a_ref.shape[1], a_ref.shape[2]
    kinds, nb = x_ref.shape[0], x_ref.shape[1]
    half = nb // 2
    tiles = flat // LANES
    fold = tiles // 2
    hrows = rows // 2
    pairs = n // 2
    cols = out_ref.shape[2]
    g, me = lax.axis_index("grp"), lax.axis_index("row")

    def rdma(src, dst, ssem, rsem, dev):
        return pltpu.make_async_remote_copy(
            src_ref=src, dst_ref=dst, send_sem=ssem, recv_sem=rsem,
            device_id=dev, device_id_type=pl.DeviceIdType.MESH,
        )

    def row_peer(d):
        return lax.rem(me + d, n)

    def grp_peer(d):
        return lax.rem(g + d, ng)

    barrier = pltpu.get_barrier_semaphore()
    for d in range(1, n):
        pl.semaphore_signal(
            barrier, inc=1, device_id=(g, row_peer(d)), device_id_type=pl.DeviceIdType.MESH
        )
    for d in range(1, ng):
        pl.semaphore_signal(
            barrier, inc=1, device_id=(grp_peer(d), me), device_id_type=pl.DeviceIdType.MESH
        )

    loads = [
        pltpu.make_async_copy(src, dst, in_sem.at[k])
        for k, (src, dst) in enumerate((
            (a_hbm, a_ref), (touched_hbm, touched_v), (slot_hbm, slot_v),
            (touched_hbm, touched_s), (x_hbm, x_ref), (z_hbm, z_ref),
        ))
    ]
    for c in loads:
        c.start()

    lane = iota((rows, LANES), 1)
    in_row = lax.rem(lane, nb)
    second = (lane >= nb).astype(I32)

    def pack(top, bottom, t):
        turned = pltpu.roll(bottom, LANES - half, 1)
        return jnp.where(in_row < 2 * t + second, turned, top)

    def diagonal(bottom, t):
        hit = in_row == half + 2 * t + second
        return jnp.where(hit, bottom, 0.0)

    for c in loads[:3]:
        c.wait()
    extra = jnp.zeros((rows, LANES), F32)
    for t in range(fold):
        top = a_ref[0, :, t * LANES:(t + 1) * LANES].astype(F32)
        bottom = a_ref[0, :, (t + fold) * LANES:(t + fold + 1) * LANES].astype(F32)
        gath[me, :, t * LANES:(t + 1) * LANES] = pack(top, bottom, t).astype(BF16)
        extra = extra + diagonal(bottom, t)
    gath[me, :, fold * LANES:(fold + 1) * LANES] = extra.astype(BF16)

    core = lax.rem(me, 2)
    meta[me] = jnp.full((8, LANES), -1, I32)
    meta[me, 0:1, 0:rows] = touched_v[...]
    meta[me, 1:2, 0:rows] = slot_v[...]
    own_meta = meta[me]
    own_touched = own_meta[0:1, :]
    own_slot = own_meta[1:2, :]
    meta[me] = jnp.where(core == 1, pltpu.roll(own_meta, rows, 1), own_meta)

    pl.semaphore_wait(barrier, n - 1 + ng - 1)

    started = []

    def go(src, dst, ssem, rsem, dev):
        c = rdma(src, dst, ssem, rsem, dev)
        c.start()
        started.append(c)

    counter = [0]

    def send_half(s, h, dst_row):
        k = counter[0]
        counter[0] += 1
        view = gath.at[s, pl.ds(h * hrows, hrows)]
        go(view, view, g_send.at[k], g_recv.at[s, h], (g, dst_row))

    def wait_half(s, h):
        view = gath.at[s, pl.ds(h * hrows, hrows)]
        rdma(view, view, g_send.at[0], g_recv.at[s, h], (g, row_peer(1))).wait_recv()

    relay = n == 8
    if relay:
        def flip(v, bit):
            return v + bit - 2 * bit * lax.rem(lax.div(v, bit), 2)
        sib, xn, yn = flip(me, 1), flip(me, 2), flip(me, 4)
        dn = flip(xn, 4)
        send_half(me, 0, xn)
        send_half(me, 1, yn)
        send_half(me, 1, xn)
        send_half(me, 0, yn)
        send_half(me, 0, sib)
        send_half(me, 1, sib)
    else:
        for d in range(1, n):
            for h in range(2):
                send_half(me, h, row_peer(d))
    for d in range(1, n):
        go(meta.at[me], meta.at[me], m_send.at[d], m_recv.at[me], (g, row_peer(d)))

    for c in loads[3:]:
        c.wait()

    r64, c64 = iota((nb, nb), 0), iota((nb, nb), 1)
    dup = onehot(lax.rem(iota((nb, LANES), 1), nb) == iota((nb, LANES), 0))
    lane_b = iota((nb, LANES), 1)
    for k in range(kinds):
        active = half * (1 + class_s[k])
        inside = (r64 < active) & (c64 < active)
        xm = jnp.where(inside, x_ref[k].astype(F32), 0.0).astype(BF16)
        zm_ref[k] = jnp.where(inside, z_ref[k].astype(F32), 0.0).astype(BF16)
        wide = mm(xm, dup)
        w_ref[0:nb, k * LANES:(k + 1) * LANES] = jnp.where(lane_b < nb, wide, 0.0).astype(BF16)
        w_ref[nb:2 * nb, k * LANES:(k + 1) * LANES] = jnp.where(lane_b >= nb, wide, 0.0).astype(BF16)

    spread = jnp.broadcast_to(own_touched, (LANES, LANES)).astype(F32)
    own_kind = jnp.transpose(spread)[0:rows, :]

    low_half = iota((hrows, LANES), 1) < nb
    group = 4

    def left_tiles(u, carry):
        tiles_in = [
            a_ref[0, :, pl.ds(pl.multiple_of((u * group + v) * LANES, LANES), LANES)]
            for v in range(group)
        ]
        at = jnp.concatenate(tiles_in, axis=0)
        acc = [jnp.zeros((rows, LANES), F32) for _ in range(group)]
        for k in range(0, kinds, 2):
            full = mm(at, w_ref[:, k * LANES:(k + 2) * LANES])
            for j in range(2):
                hit = own_kind == k + j
                for v in range(group):
                    part = full[v * rows:(v + 1) * rows, j * LANES:(j + 1) * LANES]
                    acc[v] = jnp.where(hit, part, acc[v])
        for v in range(group):
            t = u * group + v
            val = acc[v].astype(BF16).astype(F32)
            top, bot = val[0:hrows], val[hrows:rows]
            even = jnp.where(low_half, top, pltpu.roll(bot, nb, 1))
            odd = jnp.where(low_half, pltpu.roll(top, nb, 1), bot)
            l3[pl.ds(2 * t, hrows, stride=nb), :] = even
            l3[pl.ds(2 * t + 1, hrows, stride=nb), :] = odd
        return carry

    lax.fori_loop(0, tiles // group, left_tiles, 0)

    i0, i1 = iota((LANES, LANES), 0), iota((LANES, LANES), 1)
    same = (i0 < nb) == (i1 < nb)
    on_diag = lax.rem(iota((nb, LANES), 1), nb) == iota((nb, LANES), 0)
    unroll = 4

    def product_step(u, carry):
        for v in range(unroll):
            i = u * unroll + v
            off = pl.multiple_of(i * nb, nb)
            lt = l3[pl.ds(off, nb), :].astype(BF16)
            zk = jnp.concatenate(
                [zm_ref[touched_s[0, i]], zm_ref[touched_s[0, i + hrows]]], axis=0
            )
            pt = jnp.where(same, mm(zk, lt), 0.0).astype(BF16)
            ptf = pt[0:nb].astype(F32) + pt[nb:2 * nb].astype(F32)
            p3[pl.ds(off, nb), :] = jnp.where(on_diag, ptf, ptf + mm_nt(dup, pt))
        return carry

    steps = hrows // unroll
    if relay:
        lax.fori_loop(0, steps // 2, product_step, 0)
        wait_half(xn, 0)
        send_half(xn, 0, yn)
        send_half(xn, 0, sib)
        wait_half(yn, 1)
        send_half(yn, 1, xn)
        send_half(yn, 1, sib)
        lax.fori_loop(steps // 2, steps, product_step, 0)
        wait_half(xn, 1)
        send_half(xn, 1, sib)
        wait_half(yn, 0)
        send_half(yn, 0, sib)
    else:
        lax.fori_loop(0, steps, product_step, 0)

    qextra = jnp.zeros((rows, LANES), F32)

    def put(t, v):
        hi, lo = split(v)
        q_ref[0:rows, t * LANES:(t + 1) * LANES] = hi
        q_ref[rows:2 * rows, t * LANES:(t + 1) * LANES] = lo

    def flat_tile(t):
        even = p3[pl.ds(2 * t, hrows, stride=nb), :]
        odd = p3[pl.ds(2 * t + 1, hrows, stride=nb), :]
        top = jnp.where(low_half, even, pltpu.roll(odd, nb, 1))
        bot = jnp.where(low_half, pltpu.roll(even, nb, 1), odd)
        return jnp.concatenate([top, bot], axis=0)

    for t in range(fold):
        top, bottom = flat_tile(t), flat_tile(t + fold)
        put(t, pack(top, bottom, t))
        qextra = qextra + diagonal(bottom, t)
    put(fold, qextra)

    for d in range(1, n):
        s = row_peer(d)
        rdma(meta.at[s], meta.at[s], m_send.at[d], m_recv.at[s], (g, s)).wait_recv()

    def pair_meta(p):
        return jnp.maximum(meta[2 * p], meta[2 * p + 1])

    def score_pair(p):
        block = gath[pl.ds(2 * p, 2)].reshape(2 * rows, gath.shape[2])
        s = mm_nt(q_ref[...], block)
        s = s[0:rows] + s[rows:2 * rows]
        kind = pair_meta(p)[0:1, :].astype(F32)
        score[p] = jnp.where(own_kind == kind, s, 0.0)

    mine = lax.div(me, 2)
    if relay:
        wait_half(sib, 0)
        wait_half(sib, 1)
        score_pair(mine)
        sx, sy, sd = flip(sib, 2), flip(sib, 4), flip(flip(sib, 2), 4)
        wait_half(sx, 0)
        wait_half(sx, 1)
        score_pair(lax.div(xn, 2))
        wait_half(dn, 0)
        send_half(dn, 0, sib)
        wait_half(dn, 1)
        send_half(dn, 1, sib)
        wait_half(sy, 0)
        wait_half(sy, 1)
        score_pair(lax.div(yn, 2))
        wait_half(sd, 0)
        wait_half(sd, 1)
        score_pair(lax.div(dn, 2))
    else:
        for d in range(1, n):
            for h in range(2):
                wait_half(row_peer(d), h)

        def each(p, carry):
            score_pair(p)
            return carry

        lax.fori_loop(0, pairs, each, 0)

    def column_slice(q):
        def body(p, acc):
            want = q * cols + iota((cols, LANES), 0)
            table = onehot(pair_meta(p)[1:2, :] == want)
            hi, lo = split(score[p])
            both = mm_nt(jnp.concatenate([hi, lo], axis=0), table)
            return acc + both[0:rows] + both[rows:2 * rows]
        acc = jnp.zeros((rows, cols), F32)
        if pairs <= 4:
            for p in range(pairs):
                acc = body(p, acc)
            return acc
        return lax.fori_loop(0, pairs, body, acc)

    for d in range(1, ng):
        q = grp_peer(d)
        zsend[d] = column_slice(q)
        go(zsend.at[d], zrecv.at[g], z_ssem.at[d], z_rsem.at[g], (q, me))
    total = column_slice(g)

    before = onehot((i0 < i1) & ((i0 < rows) == (i1 < rows)))
    o_id = iota((n, LANES), 0)
    owner = (own_slot >= o_id * rows) & (own_slot < (o_id + 1) * rows)
    owner_f = jnp.where(owner, 1.0, 0.0)
    rank = mm(onehot(owner), before)
    place = jnp.where(owner, rank + (o_id * cap).astype(F32) + 1.0, 0.0)
    place = jnp.sum(place, axis=0, keepdims=True).astype(I32) - 1
    route = onehot(iota((n * cap, LANES), 0) == place)[:, 0:rows]

    def landing(p):
        slots = pair_meta(p)[1:2, :]
        arrives = (slots >= me * rows) & (slots < (me + 1) * rows)
        arr = jnp.broadcast_to(jnp.where(arrives, 1.0, 0.0), (8, LANES)).astype(BF16)
        rank_in = mm(arr, before)[0:1, :].astype(I32)
        upper = (iota((1, LANES), 1) >= rows).astype(I32)
        at = jnp.where(arrives, rank_in + upper * cap, -1)
        pick = onehot(iota((2 * cap, LANES), 0) == at)
        where_to = onehot(slots == me * rows + iota((rows, LANES), 0))
        return mm_nt(where_to, pick).astype(BF16)

    lands = [landing(p) for p in range(pairs)]

    for d in range(1, ng):
        s = grp_peer(d)
        rdma(zsend.at[d], zrecv.at[s], z_ssem.at[d], z_rsem.at[s], (s, me)).wait_recv()
        total = total + zrecv[s]

    hi, lo = split(total)
    osend[...] = (mm(route, hi) + mm(route, lo)).reshape(osend.shape)
    for d in range(1, n):
        o = row_peer(d)
        go(osend.at[o], orecv.at[me], o_send.at[d], o_recv.at[me], (g, o))
    orecv[me] = osend[me]
    for d in range(1, n):
        s = row_peer(d)
        rdma(osend.at[s], orecv.at[s], o_send.at[d], o_recv.at[s], (g, s)).wait_recv()
    high = jnp.zeros((rows, cols), F32)
    low = jnp.zeros((rows, cols), F32)
    for p in range(pairs):
        hi, lo = split(orecv[2 * p:2 * p + 2].reshape(2 * cap, cols))
        high = high + mm(lands[p], hi)
        low = low + mm(lands[p], lo)
    out_ref[0] = high
    out_ref[1] = low
    for c in started:
        c.wait_send()


def shards(n, ng, a_pieces, touched, slot_row, x_blocks, z_inverse, block_class):
    rows, flat = a_pieces.shape[1], a_pieces.shape[2]
    kinds, nb = x_blocks.shape[0], x_blocks.shape[1]
    packed = (flat // LANES // 2 + 1) * LANES
    cols = rows * n // ng
    cap = -(-max(2, rows // n * 2) // 8) * 8
    sends = 14 if n == 8 else 2 * n
    vmem = pl.BlockSpec(memory_space=pltpu.VMEM)
    hbm = pl.BlockSpec(memory_space=pl.ANY)
    smem = pl.BlockSpec(memory_space=pltpu.SMEM)
    dma = pltpu.SemaphoreType.DMA
    parts = pl.pallas_call(
        functools.partial(kernel, n, ng, cap),
        out_shape=jax.ShapeDtypeStruct((2, rows, cols), F32),
        in_specs=[hbm, hbm, smem, hbm, hbm, hbm],
        out_specs=vmem,
        scratch_shapes=[
            pltpu.VMEM(a_pieces.shape, BF16),
            pltpu.SMEM(touched.shape, I32),
            pltpu.VMEM(touched.shape, I32),
            pltpu.VMEM((1, rows), I32),
            pltpu.VMEM(x_blocks.shape, BF16),
            pltpu.VMEM(z_inverse.shape, BF16),
            dma((6,)),
            pltpu.VMEM((n, rows, packed), BF16),
            pltpu.VMEM((n, 8, LANES), I32),
            pltpu.VMEM((2 * nb, kinds * LANES), BF16),
            pltpu.VMEM((kinds, nb, nb), BF16),
            pltpu.VMEM((rows // 2 * nb, LANES), F32),
            pltpu.VMEM((rows // 2 * nb, LANES), F32),
            pltpu.VMEM((2 * rows, packed), BF16),
            pltpu.VMEM((n // 2, rows, LANES), F32),
            pltpu.VMEM((ng, rows, cols), F32),
            pltpu.VMEM((ng, rows, cols), F32),
            pltpu.VMEM((n, cap, cols), F32),
            pltpu.VMEM((n, cap, cols), F32),
            dma((sends,)), dma((n, 2)), dma((n,)), dma((n,)),
            dma((ng,)), dma((ng,)), dma((n,)), dma((n,)),
        ],
        compiler_params=pltpu.CompilerParams(
            collective_id=0, has_side_effects=True, vmem_limit_bytes=56 * 1024 * 1024
        ),
    )(a_pieces, touched, block_class, slot_row.reshape(1, rows), x_blocks, z_inverse)
    return parts[0] + parts[1]


def solution(mesh):
    n, ng = mesh.shape["row"], mesh.shape["grp"]
    return jax.shard_map(
        functools.partial(shards, n, ng),
        mesh=mesh,
        in_specs=(
            P("grp", "row", None),
            P("grp", "row"),
            P("row"),
            P("grp", None, None),
            P("grp", None, None),
            P("grp"),
        ),
        out_specs=P("row", "grp"),
        check_vma=False,
    )
```
